32 devices in a mesh: dp: 1 (over z), vp: 32 (over y, x, core).
Axes of the slice: x: 4, y: 4, z: 1, core: 2. Of those that a mesh axis runs over, the one named last changes fastest.
The devices are a block of a 4x4x8 slice.
Arguments:
- hidden: bfloat16 [1024, 4096], P('dp')
- w_head: bfloat16 [4096, 128256], P(None, 'vp')
- inv_temp: float32 [1024], P('dp')
- target: int32 [1024], P('dp')
Outputs:
- output 1: float32 [1024, 128256], P('dp', 'vp')
- output 2: float32 [1024], P('dp')
All inputs are finite; a program needn't handle non-finite values.
Results may differ from the reference program's by a relative error of at most 0.001.
Values are sent between devices in bfloat16 or wider.
A program may use at most 768 MiB of HBM per device.

```python
import math
import jax
import jax.numpy as jnp

ROWS = 1024
D = 4096
V = 128256


def setup_inputs(seed: int = 0, part: int = 0) -> dict:
    shared_key = jax.random.key(seed)
    key_wnoise, key_wlead = jax.random.split(shared_key)
    part_key = jax.random.fold_in(jax.random.key(seed + 1), part)
    key_hidden, key_lead, key_temp, key_target = jax.random.split(part_key, 4)
    lead_dims = 4
    ramp = 1.0 - 2.0 * jnp.arange(V, dtype=jnp.float32) / (V - 1)
    w_lead = 0.5 * ramp[None, :] * (1.0 + 0.25 * jax.random.normal(key_wlead, (lead_dims, V), jnp.float32))
    w_rest = jax.random.normal(key_wnoise, (D - lead_dims, V), jnp.float32) * (D ** -0.5)
    w_head = jnp.concatenate([w_lead, w_rest], axis=0).astype(jnp.bfloat16)
    h_lead = 1.0 + 0.3 * jax.random.normal(key_lead, (ROWS, lead_dims), jnp.float32)
    h_rest = jax.random.normal(key_hidden, (ROWS, D - lead_dims), jnp.float32)
    hidden = jnp.concatenate([h_lead, h_rest], axis=1).astype(jnp.bfloat16)
    inv_temp = jnp.exp(jax.random.uniform(key_temp, (ROWS,), jnp.float32, math.log(0.5), math.log(16.0)))
    low_id = V // 4
    target = jax.random.randint(key_target, (ROWS,), low_id, V, jnp.int32)
    target = target.at[0].set(low_id).at[1].set(V - 1)
    return {"hidden": hidden, "w_head": w_head, "inv_temp": inv_temp, "target": target}


def reference(hidden, w_head, inv_temp, target):
    logits = jnp.dot(hidden, w_head, preferred_element_type=jnp.float32) * inv_temp[:, None]
    row_max = jnp.max(logits, axis=1, keepdims=True)
    exp_vals = jnp.exp(logits - row_max)
    row_total = jnp.sum(exp_vals, axis=1, keepdims=True)
    cdf_table = jnp.cumsum(exp_vals / row_total, axis=1)
    cdf_target = jnp.take_along_axis(cdf_table, target[:, None], axis=1)[:, 0]
    return cdf_table, cdf_target
```

```python
import functools
import math
import jax
import jax.numpy as jnp
from jax import lax
from jax.experimental import pallas as pl
from jax.experimental.pallas import tpu as pltpu
from jax.sharding import PartitionSpec as P

LOG2E = math.log2(math.e)
LANES = 128
SUBLANES = 8
CHUNK = 512
SEG = 128
UNIT = 256
FIRST_UNITS = 2


def exp_of(x):
    return jnp.exp2(x * LOG2E)


def spread(row):
    return jnp.broadcast_to(row, (SUBLANES, LANES))


def main_kernel(wt_hbm, h_hbm, tau_ref, tgt_ref, c_ref, stat_ref, mh,
                w_v, h_v, z_v, m_st, s_st, t_st, w_sem, h_sem):
    me = lax.axis_index("vp")
    width, depth = wt_hbm.shape
    rows = h_hbm.shape[0]
    units = rows // UNIT
    groups = UNIT // LANES
    n_chunk = pl.cdiv(width, CHUNK)
    n_seg = mh.shape[0]

    def size_of(s):
        return min(CHUNK, width - s * CHUNK)

    def h_copy(u):
        r = pl.ds(u * UNIT, UNIT)
        return pltpu.make_async_copy(h_hbm.at[r, :], h_v.at[r, :], h_sem.at[u])

    def w_copy(s):
        v = pl.ds(s * CHUNK, size_of(s))
        return pltpu.make_async_copy(wt_hbm.at[v, :], w_v.at[v, :], w_sem.at[s])

    for u in range(FIRST_UNITS):
        h_copy(u).start()
    for s in range(n_chunk):
        w_copy(s).start()
    for u in range(FIRST_UNITS, units):
        h_copy(u).start()

    sub = lax.broadcasted_iota(jnp.int32, (SUBLANES, LANES), 0)

    m_st[...] = jnp.full_like(m_st, -jnp.inf)
    s_st[...] = jnp.zeros_like(s_st)
    t_st[...] = jnp.zeros_like(t_st)

    def prefix(x):
        for step in (1, 2, 4):
            x = x + jnp.where(sub >= step, pltpu.roll(x, step, axis=0), 0.0)
        return x

    def all_sublanes(op, x):
        for step in (4, 2, 1):
            x = op(x, pltpu.roll(x, step, axis=0))
        return x

    def aligned(x):
        return x if isinstance(x, int) else pl.multiple_of(x, LANES)

    def epilogue(r0, nr, s, slot):
        for g in range(nr // LANES):
            rg = r0 // LANES + g
            lanes = pl.ds(aligned(r0 + g * LANES), LANES)
            tau = spread(tau_ref[pl.ds(rg, 1), :])
            tgt = spread(tgt_ref[pl.ds(rg, 1), :]) - me * width
            m = m_st[:, lanes]
            run = s_st[:, lanes]
            tacc = t_st[:, lanes]
            for j in range(pl.cdiv(size_of(s), SEG)):
                v0 = s * CHUNK + j * SEG
                used = min(SEG, width - v0) // SUBLANES
                zt = [z_v[slot, j * SEG + i * SUBLANES:j * SEG + (i + 1) * SUBLANES,
                          g * LANES:(g + 1) * LANES] * tau for i in range(used)]
                bm = zt
                while len(bm) > 1:
                    bm = [jnp.maximum(*bm[i:i + 2]) if i + 1 < len(bm) else bm[i] for i in range(0, len(bm), 2)]
                m_new = jnp.maximum(m, all_sublanes(jnp.maximum, bm[0]))
                alpha = exp_of(m - m_new)
                m = m_new
                run = run * alpha
                tacc = tacc * alpha
                for i in range(used):
                    pre = prefix(exp_of(zt[i] - m))
                    cur = pre + run
                    run = run + spread(pre[SUBLANES - 1:SUBLANES, :])
                    tacc = tacc + jnp.where(sub == tgt - (v0 + i * SUBLANES), cur, 0.0)
                    c_ref[v0 + i * SUBLANES:v0 + (i + 1) * SUBLANES, lanes] = cur
                mh[v0 // SEG:v0 // SEG + 1, lanes] = m[0:1, :]
            m_st[:, lanes] = m
            s_st[:, lanes] = run
            t_st[:, lanes] = tacc

    def pack_stats(u):
        for g in range(groups):
            rg = u * groups + g
            lanes = pl.ds(aligned(rg * LANES), LANES)
            stat_ref[0, pl.ds(rg, 1), :] = m_st[0:1, lanes]
            stat_ref[1, pl.ds(rg, 1), :] = s_st[0:1, lanes]
            stat_ref[2, pl.ds(rg, 1), :] = all_sublanes(jnp.add, t_st[:, lanes])[0:1, :]

    def dot_tile(r0, nr, s, slot, lane0=0):
        c0, size = s * CHUNK, size_of(s)
        z_v[slot, 0:size, lane0:lane0 + nr] = lax.dot_general(
            w_v[c0:c0 + size, :], h_v[pl.ds(r0, nr), :], (((1,), (1,)), ((), ())),
            preferred_element_type=jnp.float32)

    last = n_chunk - 1
    first_rows = FIRST_UNITS * UNIT
    for u in range(FIRST_UNITS):
        h_copy(u).wait()
    for s in range(last):
        w_copy(s).wait()
        if s > 0:
            epilogue(0, first_rows, s - 1, (s - 1) % 2)
        dot_tile(0, first_rows, s, s % 2)
    w_copy(last).wait()
    epilogue(0, first_rows, last - 1, (last - 1) % 2)
    for u in range(FIRST_UNITS):
        if u > 0:
            epilogue((u - 1) * UNIT, UNIT, last, (last + u - 1) % 2)
            pack_stats(u - 1)
        dot_tile(u * UNIT, UNIT, last, (last + u) % 2)
    lag = (last + FIRST_UNITS - 1) % 2

    def unit(u, carry):
        r0 = pl.multiple_of(u * UNIT, UNIT)
        h_copy(u).wait()
        epilogue(r0 - UNIT, UNIT, last, lag)
        pack_stats(u - 1)
        for s in range(n_chunk):
            slot = (lag + 1 + s) % 2
            if s > 0:
                epilogue(r0, UNIT, s - 1, 1 - slot)
            dot_tile(r0, UNIT, s, slot)
        return carry

    lax.fori_loop(FIRST_UNITS, units, unit, 0)
    epilogue((units - 1) * UNIT, UNIT, last, (lag + 1 + last) % 2)
    pack_stats(units - 1)


def exchange_kernel(n, width, stat_ref, mh_ref, tgt_ref, ab_ref, ct_ref, recv_v, send_sem, recv_sem):
    me = lax.axis_index("vp")
    n_seg = mh_ref.shape[0]
    n_rg = tgt_ref.shape[0]
    barrier = pltpu.get_barrier_semaphore()

    def peer(k):
        return {"vp": lax.rem(me + k, n)}

    def greet(k, carry):
        pl.semaphore_signal(barrier, inc=1, device_id=peer(k), device_id_type=pl.DeviceIdType.MESH)
        return carry

    def copy(k):
        return pltpu.make_async_remote_copy(
            src_ref=stat_ref, dst_ref=recv_v.at[k - 1], send_sem=send_sem.at[k - 1], recv_sem=recv_sem.at[k - 1],
            device_id=peer(k), device_id_type=pl.DeviceIdType.MESH)

    def send(k, carry):
        copy(k).start()
        return carry

    def wait_recv(k, carry):
        copy(k).wait_recv()
        return carry

    def wait_send(k, carry):
        copy(k).wait_send()
        return carry

    lax.fori_loop(1, n, greet, 0)
    pl.semaphore_wait(barrier, n - 1)
    lax.fori_loop(1, n, send, 0)
    lax.fori_loop(1, n, wait_recv, 0)

    gm = stat_ref[0]
    for k in range(1, n):
        gm = jnp.maximum(gm, recv_v[k - 1, 0])
    tgt = tgt_ref[...]
    f = exp_of(stat_ref[0] - gm)
    sc = stat_ref[1] * f
    total = sc
    before = jnp.zeros_like(sc)
    hit = stat_ref[2] * f + jnp.where((me + 1) * width <= tgt, sc, 0.0)
    for k in range(1, n):
        f = exp_of(recv_v[k - 1, 0] - gm)
        sc = recv_v[k - 1, 1] * f
        src = lax.rem(me + n - k, n)
        total = total + sc
        before = before + jnp.where(src < me, sc, 0.0)
        hit = hit + recv_v[k - 1, 2] * f + jnp.where((src + 1) * width <= tgt, sc, 0.0)
    ct_ref[...] = hit / total
    off = before / total
    for g in range(n_rg):
        lanes = slice(g * LANES, (g + 1) * LANES)
        ab_ref[0:n_seg, lanes] = exp_of(mh_ref[:, lanes] - gm[g:g + 1, :]) / total[g:g + 1, :]
        ab_ref[n_seg:n_seg + 1, lanes] = off[g:g + 1, :]
    lax.fori_loop(1, n, wait_send, 0)


def table_kernel(c_ref, ab_ref, ct_ref, out_hbm, ct_out, stage, sem):
    width, rows = out_hbm.shape
    ct_out[...] = ct_ref[...]
    n_seg = pl.cdiv(width, SEG)

    def copy(t):
        v = pl.ds(t * SEG, min(SEG, width - t * SEG))
        return pltpu.make_async_copy(stage.at[v, :], out_hbm.at[v, :], sem.at[t])

    for t in range(n_seg):
        v0 = t * SEG
        size = min(SEG, width - v0)
        stage[v0:v0 + size, :] = c_ref[v0:v0 + size, :] * ab_ref[t:t + 1, :] + ab_ref[n_seg:n_seg + 1, :]
        copy(t).start()
    for t in range(n_seg):
        copy(t).wait()


def solution(mesh):
    n = mesh.shape["vp"]

    def local_fn(h_rows, w_cols, tau_rows, tgt_rows):
        rows, depth = h_rows.shape
        width = w_cols.shape[1]
        units = rows // UNIT
        n_rg = rows // LANES
        n_seg = pl.cdiv(width, SEG)
        ab_rows = pl.cdiv(n_seg + 1, SUBLANES) * SUBLANES
        vmem = pl.BlockSpec(memory_space=pltpu.VMEM)
        hbm = pl.BlockSpec(memory_space=pl.ANY)
        tau2, tgt2 = tau_rows.reshape(n_rg, LANES), tgt_rows.reshape(n_rg, LANES)
        c, stat, mh = pl.pallas_call(
            main_kernel,
            name="main_kernel",
            out_shape=(pltpu.VMEM((width, rows), jnp.float32),
                       pltpu.VMEM((3, n_rg, LANES), jnp.float32),
                       pltpu.VMEM((n_seg, rows), jnp.float32)),
            in_specs=[hbm, hbm, vmem, vmem],
            out_specs=(vmem, vmem, vmem),
            scratch_shapes=[
                pltpu.VMEM((width, depth), jnp.bfloat16),
                pltpu.VMEM((rows, depth), jnp.bfloat16),
                pltpu.VMEM((2, CHUNK, FIRST_UNITS * UNIT), jnp.float32),
                pltpu.VMEM((SUBLANES, rows), jnp.float32),
                pltpu.VMEM((SUBLANES, rows), jnp.float32),
                pltpu.VMEM((SUBLANES, rows), jnp.float32),
                pltpu.SemaphoreType.DMA((pl.cdiv(width, CHUNK),)),
                pltpu.SemaphoreType.DMA((units,)),
            ],
            compiler_params=pltpu.CompilerParams(vmem_limit_bytes=45 * 1024 * 1024),
        )(w_cols.T, h_rows, tau2, tgt2)
        stat, mh, c = (pltpu.with_memory_space_constraint(x, pltpu.VMEM) for x in (stat, mh, c))
        ab, ct = pl.pallas_call(
            functools.partial(exchange_kernel, n, width),
            name="exchange_kernel",
            out_shape=(pltpu.VMEM((ab_rows, rows), jnp.float32), pltpu.VMEM((n_rg, LANES), jnp.float32)),
            in_specs=[vmem, vmem, vmem],
            out_specs=(vmem, vmem),
            scratch_shapes=[
                pltpu.VMEM((n - 1, 3, n_rg, LANES), jnp.float32),
                pltpu.SemaphoreType.DMA((n - 1,)),
                pltpu.SemaphoreType.DMA((n - 1,)),
            ],
            compiler_params=pltpu.CompilerParams(
                collective_id=0, has_side_effects=True, vmem_limit_bytes=4 * 1024 * 1024),
        )(stat, mh, tgt2)
        table, ct2 = pl.pallas_call(
            table_kernel,
            name="table_kernel",
            out_shape=(jax.ShapeDtypeStruct((width, rows), jnp.float32),
                       jax.ShapeDtypeStruct((n_rg, LANES), jnp.float32)),
            in_specs=[vmem, vmem, vmem],
            out_specs=(hbm, vmem),
            scratch_shapes=[pltpu.VMEM((width, rows), jnp.float32),
                            pltpu.SemaphoreType.DMA((n_seg,))],
            compiler_params=pltpu.CompilerParams(vmem_limit_bytes=20 * 1024 * 1024),
        )(*(pltpu.with_memory_space_constraint(x, pltpu.VMEM) for x in (c, ab, ct)))
        return table.T, ct2.reshape(rows)

    return jax.shard_map(
        local_fn,
        mesh=mesh,
        in_specs=(P("dp", None), P(None, "vp"), P("dp"), P("dp")),
        out_specs=(P("dp", "vp"), P("dp")),
        check_vma=False,
    )
```

```python
import functools
import math
import jax
import jax.numpy as jnp
from jax import lax
from jax.experimental import pallas as pl
from jax.experimental.pallas import tpu as pltpu
from jax.sharding import PartitionSpec as P

LOG2E = math.log2(math.e)
LANES = 128
SUBLANES = 8
CHUNK = 512
SEG = 128
PIECE = 64
UNIT = 256
FIRST_UNITS = 2


def exp_of(x):
    return jnp.exp2(x * LOG2E)


def spread(row):
    return jnp.broadcast_to(row, (SUBLANES, LANES))


def main_kernel(wt_hbm, h_hbm, tau_ref, tgt_ref, c_ref, stat_ref, mh,
                w_v, h_v, z_v, m_st, s_st, t_st, w_sem, h_sem):
    me = lax.axis_index("vp")
    width, depth = wt_hbm.shape
    rows = h_hbm.shape[0]
    units = rows // UNIT
    groups = UNIT // LANES
    n_chunk = pl.cdiv(width, CHUNK)
    n_seg = mh.shape[0]

    def size_of(s):
        return min(CHUNK, width - s * CHUNK)

    def h_copy(u):
        r = pl.ds(u * UNIT, UNIT)
        return pltpu.make_async_copy(h_hbm.at[r, :], h_v.at[r, :], h_sem.at[u])

    def w_copy(s):
        v = pl.ds(s * CHUNK, size_of(s) if isinstance(s, int) else CHUNK)
        return pltpu.make_async_copy(wt_hbm.at[v, :], w_v.at[v, :], w_sem.at[s])

    def start(src, dst, sem, r0, nr):
        def piece(i, carry):
            r = pl.ds(pl.multiple_of(r0 + i * PIECE, SUBLANES), PIECE)
            pltpu.make_async_copy(src.at[r, :], dst.at[r, :], sem).start()
            return carry
        lax.fori_loop(0, nr // PIECE, piece, 0)
        rest = nr % PIECE
        if rest:
            r = pl.ds(r0 + nr - rest, rest)
            pltpu.make_async_copy(src.at[r, :], dst.at[r, :], sem).start()

    def start_h(u):
        start(h_hbm, h_v, h_sem.at[u], u * UNIT, UNIT)

    def start_w(s):
        start(wt_hbm, w_v, w_sem.at[s], s * CHUNK, size_of(s))

    for u in range(FIRST_UNITS):
        start_h(u)
    start_w(0)
    for u in range(FIRST_UNITS, units):
        start_h(u)
    for s in range(1, n_chunk):
        start_w(s)

    sub = lax.broadcasted_iota(jnp.int32, (SUBLANES, LANES), 0)

    m_st[...] = jnp.full_like(m_st, -jnp.inf)
    s_st[...] = jnp.zeros_like(s_st)
    t_st[...] = jnp.zeros_like(t_st)

    def prefix(x):
        for step in (1, 2, 4):
            x = x + jnp.where(sub >= step, pltpu.roll(x, step, axis=0), 0.0)
        return x

    def all_sublanes(op, x):
        for step in (4, 2, 1):
            x = op(x, pltpu.roll(x, step, axis=0))
        return x

    def aligned(x):
        return x if isinstance(x, int) else pl.multiple_of(x, LANES)

    def epilogue(r0, nr, s, slot):
        for g in range(nr // LANES):
            rg = r0 // LANES + g
            lanes = pl.ds(aligned(r0 + g * LANES), LANES)
            tau = spread(tau_ref[pl.ds(rg, 1), :])
            tgt = spread(tgt_ref[pl.ds(rg, 1), :]) - me * width
            m = m_st[:, lanes]
            run = s_st[:, lanes]
            tacc = t_st[:, lanes]
            for j in range(pl.cdiv(size_of(s), SEG)):
                v0 = s * CHUNK + j * SEG
                used = min(SEG, width - v0) // SUBLANES
                zt = [z_v[slot, j * SEG + i * SUBLANES:j * SEG + (i + 1) * SUBLANES,
                          g * LANES:(g + 1) * LANES] * tau for i in range(used)]
                bm = zt
                while len(bm) > 1:
                    bm = [jnp.maximum(*bm[i:i + 2]) if i + 1 < len(bm) else bm[i] for i in range(0, len(bm), 2)]
                m_new = jnp.maximum(m, all_sublanes(jnp.maximum, bm[0]))
                alpha = exp_of(m - m_new)
                m = m_new
                run = run * alpha
                tacc = tacc * alpha
                for i in range(used):
                    pre = prefix(exp_of(zt[i] - m))
                    cur = pre + run
                    run = run + spread(pre[SUBLANES - 1:SUBLANES, :])
                    tacc = tacc + jnp.where(sub == tgt - (v0 + i * SUBLANES), cur, 0.0)
                    c_ref[v0 + i * SUBLANES:v0 + (i + 1) * SUBLANES, lanes] = cur
                mh[v0 // SEG:v0 // SEG + 1, lanes] = m[0:1, :]
            m_st[:, lanes] = m
            s_st[:, lanes] = run
            t_st[:, lanes] = tacc

    def pack_stats(u):
        for g in range(groups):
            rg = u * groups + g
            lanes = pl.ds(aligned(rg * LANES), LANES)
            stat_ref[0, pl.ds(rg, 1), :] = m_st[0:1, lanes]
            stat_ref[1, pl.ds(rg, 1), :] = s_st[0:1, lanes]
            stat_ref[2, pl.ds(rg, 1), :] = all_sublanes(jnp.add, t_st[:, lanes])[0:1, :]

    def dot_tile(r0, nr, s, slot, lane0=0):
        c0, size = s * CHUNK, size_of(s)
        z_v[slot, 0:size, lane0:lane0 + nr] = lax.dot_general(
            w_v[c0:c0 + size, :], h_v[pl.ds(r0, nr), :], (((1,), (1,)), ((), ())),
            preferred_element_type=jnp.float32)

    last = n_chunk - 1
    half = FIRST_UNITS * UNIT
    pending = []

    def tile(r0, nr, s):
        slot = 0
        if pending:
            done = pending.pop()
            slot = 1 - done[3]
            epilogue(*done)
        dot_tile(r0, nr, s, slot)
        pending.append((r0, nr, s, slot))

    def wait_w(s, carry):
        w_copy(s).wait()
        return carry

    def wait_h(u, carry):
        h_copy(u).wait()
        return carry

    for u in range(FIRST_UNITS):
        h_copy(u).wait()
    w_copy(0).wait()
    tile(0, half, 0)
    w_copy(1).wait()
    lax.fori_loop(FIRST_UNITS, units, wait_h, 0)
    tile(half, half, 0)
    for s in range(1, 2):
        tile(0, half, s)
        tile(half, half, s)
    lax.fori_loop(2, 4, wait_w, 0)
    for s in range(2, 4):
        tile(0, half, s)
        tile(half, half, s)
    w_copy(last).wait()
    lax.fori_loop(4, last, wait_w, 0)
    for s in range(4, last):
        tile(0, half, s)
    for u in range(FIRST_UNITS):
        tile(u * UNIT, UNIT, last)
        if u > 0:
            pack_stats(u - 1)
    lag = pending.pop()[3]

    def unit(u, carry):
        r0 = pl.multiple_of(u * UNIT, UNIT)
        pending.append((r0 - UNIT, UNIT, last, lag))
        for s in range(4, n_chunk):
            tile(r0, UNIT, s)
            if s == 4:
                pack_stats(u - 1)
        pending.pop()
        return carry

    lax.fori_loop(FIRST_UNITS, units, unit, 0)
    epilogue((units - 1) * UNIT, UNIT, last, lag)
    pack_stats(units - 1)


def exchange_kernel(n, width, stat_ref, mh_ref, tgt_ref, ab_ref, ct_ref, recv_v, send_sem, recv_sem):
    me = lax.axis_index("vp")
    n_seg = mh_ref.shape[0]
    n_rg = tgt_ref.shape[0]
    barrier = pltpu.get_barrier_semaphore()

    def peer(k):
        return {"vp": lax.rem(me + k, n)}

    def greet(k, carry):
        pl.semaphore_signal(barrier, inc=1, device_id=peer(k), device_id_type=pl.DeviceIdType.MESH)
        return carry

    def copy(k):
        return pltpu.make_async_remote_copy(
            src_ref=stat_ref, dst_ref=recv_v.at[k - 1], send_sem=send_sem.at[k - 1], recv_sem=recv_sem.at[k - 1],
            device_id=peer(k), device_id_type=pl.DeviceIdType.MESH)

    def send(k, carry):
        copy(k).start()
        return carry

    def wait_recv(k, carry):
        copy(k).wait_recv()
        return carry

    def wait_send(k, carry):
        copy(k).wait_send()
        return carry

    lax.fori_loop(1, n, greet, 0)
    pl.semaphore_wait(barrier, n - 1)
    lax.fori_loop(1, n, send, 0)
    lax.fori_loop(1, n, wait_recv, 0)

    gm = stat_ref[0]
    for k in range(1, n):
        gm = jnp.maximum(gm, recv_v[k - 1, 0])
    tgt = tgt_ref[...]
    f = exp_of(stat_ref[0] - gm)
    sc = stat_ref[1] * f
    total = sc
    before = jnp.zeros_like(sc)
    hit = stat_ref[2] * f + jnp.where((me + 1) * width <= tgt, sc, 0.0)
    for k in range(1, n):
        f = exp_of(recv_v[k - 1, 0] - gm)
        sc = recv_v[k - 1, 1] * f
        src = lax.rem(me + n - k, n)
        total = total + sc
        before = before + jnp.where(src < me, sc, 0.0)
        hit = hit + recv_v[k - 1, 2] * f + jnp.where((src + 1) * width <= tgt, sc, 0.0)
    ct_ref[...] = hit / total
    off = before / total
    for g in range(n_rg):
        lanes = slice(g * LANES, (g + 1) * LANES)
        ab_ref[0:n_seg, lanes] = exp_of(mh_ref[:, lanes] - gm[g:g + 1, :]) / total[g:g + 1, :]
        ab_ref[n_seg:n_seg + 1, lanes] = off[g:g + 1, :]
    lax.fori_loop(1, n, wait_send, 0)


def table_kernel(c_ref, ab_ref, ct_ref, out_hbm, ct_out, stage, sem):
    width, rows = out_hbm.shape
    ct_out[...] = ct_ref[...]
    n_seg = pl.cdiv(width, SEG)

    def copy(t):
        v = pl.ds(t * SEG, min(SEG, width - t * SEG))
        return pltpu.make_async_copy(stage.at[v, :], out_hbm.at[v, :], sem.at[t])

    for t in range(n_seg):
        v0 = t * SEG
        size = min(SEG, width - v0)
        stage[v0:v0 + size, :] = c_ref[v0:v0 + size, :] * ab_ref[t:t + 1, :] + ab_ref[n_seg:n_seg + 1, :]
        copy(t).start()
    for t in range(n_seg):
        copy(t).wait()


def solution(mesh):
    n = mesh.shape["vp"]

    def local_fn(h_rows, w_cols, tau_rows, tgt_rows):
        rows, depth = h_rows.shape
        width = w_cols.shape[1]
        units = rows // UNIT
        n_rg = rows // LANES
        n_seg = pl.cdiv(width, SEG)
        ab_rows = pl.cdiv(n_seg + 1, SUBLANES) * SUBLANES
        vmem = pl.BlockSpec(memory_space=pltpu.VMEM)
        hbm = pl.BlockSpec(memory_space=pl.ANY)
        tau2, tgt2 = tau_rows.reshape(n_rg, LANES), tgt_rows.reshape(n_rg, LANES)
        c, stat, mh = pl.pallas_call(
            main_kernel,
            name="main_kernel",
            out_shape=(pltpu.VMEM((width, rows), jnp.float32),
                       pltpu.VMEM((3, n_rg, LANES), jnp.float32),
                       pltpu.VMEM((n_seg, rows), jnp.float32)),
            in_specs=[hbm, hbm, vmem, vmem],
            out_specs=(vmem, vmem, vmem),
            scratch_shapes=[
                pltpu.VMEM((width, depth), jnp.bfloat16),
                pltpu.VMEM((rows, depth), jnp.bfloat16),
                pltpu.VMEM((2, CHUNK, FIRST_UNITS * UNIT), jnp.float32),
                pltpu.VMEM((SUBLANES, rows), jnp.float32),
                pltpu.VMEM((SUBLANES, rows), jnp.float32),
                pltpu.VMEM((SUBLANES, rows), jnp.float32),
                pltpu.SemaphoreType.DMA((pl.cdiv(width, CHUNK),)),
                pltpu.SemaphoreType.DMA((units,)),
            ],
            compiler_params=pltpu.CompilerParams(vmem_limit_bytes=45 * 1024 * 1024),
        )(w_cols.T, h_rows, tau2, tgt2)
        stat, mh, c = (pltpu.with_memory_space_constraint(x, pltpu.VMEM) for x in (stat, mh, c))
        ab, ct = pl.pallas_call(
            functools.partial(exchange_kernel, n, width),
            name="exchange_kernel",
            out_shape=(pltpu.VMEM((ab_rows, rows), jnp.float32), pltpu.VMEM((n_rg, LANES), jnp.float32)),
            in_specs=[vmem, vmem, vmem],
            out_specs=(vmem, vmem),
            scratch_shapes=[
                pltpu.VMEM((n - 1, 3, n_rg, LANES), jnp.float32),
                pltpu.SemaphoreType.DMA((n - 1,)),
                pltpu.SemaphoreType.DMA((n - 1,)),
            ],
            compiler_params=pltpu.CompilerParams(
                collective_id=0, has_side_effects=True, vmem_limit_bytes=4 * 1024 * 1024),
        )(stat, mh, tgt2)
        table, ct2 = pl.pallas_call(
            table_kernel,
            name="table_kernel",
            out_shape=(jax.ShapeDtypeStruct((width, rows), jnp.float32),
                       jax.ShapeDtypeStruct((n_rg, LANES), jnp.float32)),
            in_specs=[vmem, vmem, vmem],
            out_specs=(hbm, vmem),
            scratch_shapes=[pltpu.VMEM((width, rows), jnp.float32),
                            pltpu.SemaphoreType.DMA((n_seg,))],
            compiler_params=pltpu.CompilerParams(vmem_limit_bytes=20 * 1024 * 1024),
        )(*(pltpu.with_memory_space_constraint(x, pltpu.VMEM) for x in (c, ab, ct)))
        return table.T, ct2.reshape(rows)

    return jax.shard_map(
        local_fn,
        mesh=mesh,
        in_specs=(P("dp", None), P(None, "vp"), P("dp"), P("dp")),
        out_specs=(P("dp", "vp"), P("dp")),
        check_vma=False,
    )
```

```python
import functools
import math
import jax
import jax.numpy as jnp
from jax import lax
from jax.experimental import pallas as pl
from jax.experimental.pallas import tpu as pltpu
from jax.sharding import PartitionSpec as P

LOG2E = math.log2(math.e)
LANES = 128
SUBLANES = 8
CHUNK = 512
SEG = 128
UNIT = 256
PIECE = 64
HEAD_CHUNKS = 6


def exp_of(x):
    return jnp.exp2(x * LOG2E)


def spread(row):
    return jnp.broadcast_to(row, (SUBLANES, LANES))


def all_sublanes(op, x):
    for step in (4, 2, 1):
        x = op(x, pltpu.roll(x, step, axis=0))
    return x


def prefix8(x, sub, axis):
    for step in (1, 2, 4):
        x = x + jnp.where(sub >= step, pltpu.roll(x, step, axis=axis), 0.0)
    return x


def main_kernel(wt_hbm, h_hbm, tau_ref, tgt_ref, c_ref, stat_ref, st_ref, mh,
                w_v, w_t, h_lo, h_hi, z_v, m_st, s_st, t_st, w_sem, h_sem):
    me = lax.axis_index("vp")
    width, depth = wt_hbm.shape
    rows = h_hbm.shape[0]
    half = rows // 2
    units = rows // UNIT
    groups = UNIT // LANES
    n_chunk = pl.cdiv(width, CHUNK)
    last = n_chunk - 1
    head = HEAD_CHUNKS * CHUNK

    def size_of(s):
        return min(CHUNK, width - s * CHUNK)

    def start(src, s0, dst, d0, sem, nr):
        def piece(i, carry):
            off = pl.multiple_of(i * PIECE, PIECE)
            pltpu.make_async_copy(src.at[pl.ds(s0 + off, PIECE), :], dst.at[pl.ds(d0 + off, PIECE), :], sem).start()
            return carry
        lax.fori_loop(0, nr // PIECE, piece, 0)
        rest = nr % PIECE
        if rest:
            off = nr - rest
            pltpu.make_async_copy(src.at[pl.ds(s0 + off, rest), :], dst.at[pl.ds(d0 + off, rest), :], sem).start()

    def w_at(s):
        return (w_v, s * CHUNK) if s < HEAD_CHUNKS else (w_t, s * CHUNK - head)

    def h_at(r0):
        return (h_lo, r0) if r0 < half else (h_hi, r0 - half)

    def start_h(k):
        start(h_hbm, k * half, *h_at(k * half), h_sem.at[k], half)

    def wait_h(k):
        dst, _ = h_at(k * half)
        pltpu.make_async_copy(h_hbm.at[pl.ds(k * half, half), :], dst, h_sem.at[k]).wait()

    def start_w(s):
        start(wt_hbm, s * CHUNK, *w_at(s), w_sem.at[s], size_of(s))

    def wait_w(s):
        dst, d0 = w_at(s)
        pltpu.make_async_copy(wt_hbm.at[pl.ds(s * CHUNK, size_of(s)), :],
                              dst.at[pl.ds(d0, size_of(s)), :], w_sem.at[s]).wait()

    start_h(0)
    start_w(0)
    start_h(1)
    for s in range(1, n_chunk):
        start_w(s)

    sub = lax.broadcasted_iota(jnp.int32, (SUBLANES, LANES), 0)

    m_st[...] = jnp.full_like(m_st, -jnp.inf)
    s_st[...] = jnp.zeros_like(s_st)
    t_st[...] = jnp.zeros_like(t_st)

    def epilogue(r0, nr, s, slot):
        for g in range(nr // LANES):
            rg = r0 // LANES + g
            lanes = slice(r0 + g * LANES, r0 + (g + 1) * LANES)
            tau = spread(tau_ref[rg:rg + 1, :])
            tgt = spread(tgt_ref[rg:rg + 1, :]) - me * width
            m = m_st[:, lanes]
            run = s_st[:, lanes]
            tacc = t_st[:, lanes]
            for j in range(pl.cdiv(size_of(s), SEG)):
                v0 = s * CHUNK + j * SEG
                used = min(SEG, width - v0) // SUBLANES
                zt = [z_v[slot, j * SEG + i * SUBLANES:j * SEG + (i + 1) * SUBLANES,
                          g * LANES:(g + 1) * LANES] * tau for i in range(used)]
                bm = zt
                while len(bm) > 1:
                    bm = [jnp.maximum(*bm[i:i + 2]) if i + 1 < len(bm) else bm[i] for i in range(0, len(bm), 2)]
                m_new = jnp.maximum(m, all_sublanes(jnp.maximum, bm[0]))
                alpha = exp_of(m - m_new)
                m = m_new
                run = run * alpha
                tacc = tacc * alpha
                for i in range(used):
                    pre = prefix8(exp_of(zt[i] - m), sub, 0)
                    cur = pre + run
                    run = run + spread(pre[SUBLANES - 1:SUBLANES, :])
                    tacc = tacc + jnp.where(sub == tgt - (v0 + i * SUBLANES), cur, 0.0)
                    c_ref[v0 + i * SUBLANES:v0 + (i + 1) * SUBLANES, lanes] = cur
                mh[v0 // SEG:v0 // SEG + 1, lanes] = m[0:1, :]
            m_st[:, lanes] = m
            s_st[:, lanes] = run
            t_st[:, lanes] = tacc

    def dot_tile(r0, nr, s, slot):
        w, c0 = w_at(s)
        h, h0 = h_at(r0)
        z_v[slot, 0:size_of(s), 0:nr] = lax.dot_general(
            w[c0:c0 + size_of(s), :], h[h0:h0 + nr, :], (((1,), (1,)), ((), ())),
            preferred_element_type=jnp.float32)

    pending = []

    def tile(r0, nr, s):
        slot = 0
        if pending:
            done = pending.pop()
            slot = 1 - done[3]
            epilogue(*done)
        dot_tile(r0, nr, s, slot)
        pending.append((r0, nr, s, slot))

    def half_wait(k, carry):
        pltpu.make_async_copy(h_hbm.at[pl.ds(0, half // 2), :], h_hi.at[pl.ds(0, half // 2), :], h_sem.at[1]).wait()
        return carry

    def head_wait(s, carry):
        v = pl.ds(s * CHUNK, CHUNK)
        pltpu.make_async_copy(wt_hbm.at[v, :], w_v.at[v, :], w_sem.at[s]).wait()
        return carry

    def tail_wait(i, carry):
        v = pl.ds(0, CHUNK // 2)
        pltpu.make_async_copy(wt_hbm.at[v, :], w_t.at[v, :], w_sem.at[HEAD_CHUNKS + i // 2]).wait()
        return carry

    wait_h(0)
    wait_w(0)
    tile(0, half, 0)
    wait_w(1)
    lax.fori_loop(0, 2, half_wait, 0)
    tile(half, half, 0)
    tile(0, half, 1)
    tile(half, half, 1)
    lax.fori_loop(2, HEAD_CHUNKS, head_wait, 0)
    for s in range(2, HEAD_CHUNKS):
        tile(0, half, s)
        tile(half, half, s)
    wait_w(last)
    lax.fori_loop(0, 2 * (last - HEAD_CHUNKS), tail_wait, 0)
    for s in range(HEAD_CHUNKS, last):
        tile(0, half, s)
    tile(0, UNIT, last)
    tile(UNIT, UNIT, last)
    for s in range(HEAD_CHUNKS, n_chunk):
        tile(half, UNIT, s)
    epilogue(*pending.pop())

    done = (units - 1) * groups
    for rg in range(done):
        lanes = slice(rg * LANES, (rg + 1) * LANES)
        stat_ref[rg:rg + 1, :] = m_st[0:1, lanes]
        stat_ref[done + rg:done + rg + 1, :] = s_st[0:1, lanes]
        stat_ref[2 * done + rg:2 * done + rg + 1, :] = all_sublanes(jnp.add, t_st[:, lanes])[0:1, :]
    rest = slice(done * LANES, rows)
    st_ref[0] = m_st[:, rest]
    st_ref[1] = s_st[:, rest]
    st_ref[2] = t_st[:, rest]


def tail_kernel(n, width, wt_hbm, h_hbm, tau_ref, tgt_ref, stat_ref, st_ref, mh_ref, c_ref, ab_ref, ct_ref,
                w_t, h_t, w_sem, h_sem, z_v, st_v, mh_v, late_v, recv_a, recv_b, send_a, got_a, send_b, got_b):
    me = lax.axis_index("vp")
    n_rg = tgt_ref.shape[0]
    groups = UNIT // LANES
    done = n_rg - groups
    n_seg = mh_ref.shape[0]
    head_seg = HEAD_CHUNKS * CHUNK // SEG
    n_early = recv_a.shape[1]
    n_mixed = 3 * done - n_early
    tail_rows = w_t.shape[0]
    n_tail = pl.cdiv(tail_rows, CHUNK)
    barrier = pltpu.get_barrier_semaphore()

    def peer(k):
        return {"vp": lax.rem(me + k, n)}

    def greet(k, carry):
        pl.semaphore_signal(barrier, inc=1, device_id=peer(k), device_id_type=pl.DeviceIdType.MESH)
        return carry

    def early_copy(k):
        return pltpu.make_async_remote_copy(
            src_ref=stat_ref.at[pl.ds(0, n_early), :], dst_ref=recv_a.at[k - 1],
            send_sem=send_a.at[k - 1], recv_sem=got_a.at[k - 1],
            device_id=peer(k), device_id_type=pl.DeviceIdType.MESH)

    def late_copy(k):
        return pltpu.make_async_remote_copy(
            src_ref=late_v, dst_ref=recv_b.at[k - 1],
            send_sem=send_b.at[k - 1], recv_sem=got_b.at[k - 1],
            device_id=peer(k), device_id_type=pl.DeviceIdType.MESH)

    def each(f):
        def body(k, carry):
            f(k)
            return carry
        lax.fori_loop(1, n, body, 0)

    def size_of(s):
        return min(CHUNK, tail_rows - s * CHUNK)

    def start(src, s0, dst, d0, sem, nr):
        def piece(i, carry):
            off = pl.multiple_of(i * PIECE, PIECE)
            pltpu.make_async_copy(src.at[pl.ds(s0 + off, PIECE), :], dst.at[pl.ds(d0 + off, PIECE), :], sem).start()
            return carry
        lax.fori_loop(0, nr // PIECE, piece, 0)
        rest = nr % PIECE
        if rest:
            off = nr - rest
            pltpu.make_async_copy(src.at[pl.ds(s0 + off, rest), :], dst.at[pl.ds(d0 + off, rest), :], sem).start()

    def start_all():
        start(h_hbm, done * LANES, h_t, 0, h_sem, UNIT)
        for s in range(n_tail):
            start(wt_hbm, HEAD_CHUNKS * CHUNK + s * CHUNK, w_t, s * CHUNK, w_sem.at[s], size_of(s))

    def wait_h():
        pltpu.make_async_copy(h_hbm.at[pl.ds(done * LANES, UNIT), :], h_t, h_sem).wait()

    def wait_w(s):
        v = pl.ds(s * CHUNK, size_of(s))
        pltpu.make_async_copy(wt_hbm.at[pl.ds(HEAD_CHUNKS * CHUNK + s * CHUNK, size_of(s)), :],
                              w_t.at[v, :], w_sem.at[s]).wait()

    def dot_tile(s):
        z_v[s % 2, 0:size_of(s), :] = lax.dot_general(
            w_t[s * CHUNK:s * CHUNK + size_of(s), :], h_t[...], (((1,), (1,)), ((), ())),
            preferred_element_type=jnp.float32)

    def epilogue(s):
        for g in range(groups):
            rg = done + g
            lanes = slice(g * LANES, (g + 1) * LANES)
            tau = tau_ref[rg:rg + 1, :]
            tgt = tgt_ref[rg:rg + 1, :] - (me * width + HEAD_CHUNKS * CHUNK)
            m = st_v[0, :, lanes]
            run = st_v[1, :, lanes]
            tacc = st_v[2, :, lanes]
            for j in range(pl.cdiv(size_of(s), SEG)):
                v0 = s * CHUNK + j * SEG
                size = min(SEG, tail_rows - v0)
                regs = size // SUBLANES
                z = (z_v[s % 2, j * SEG:j * SEG + size, lanes] * tau).reshape(regs, SUBLANES, LANES)
                m_new = jnp.maximum(m, all_sublanes(jnp.maximum, jnp.max(z, axis=0)))
                alpha = exp_of(m - m_new)
                m = m_new
                sub = lax.broadcasted_iota(jnp.int32, (regs, SUBLANES, LANES), 1)
                pre = prefix8(exp_of(z - m[None]), sub, 1)
                ends = jnp.broadcast_to(pre[:, SUBLANES - 1:SUBLANES, :], pre.shape)
                step = 1
                while step < regs:
                    ends = ends + jnp.concatenate([jnp.zeros((step, SUBLANES, LANES), jnp.float32), ends[:-step]])
                    step *= 2
                prior = jnp.concatenate([jnp.zeros((1, SUBLANES, LANES), jnp.float32), ends[:-1]])
                cur = pre + (prior + (run * alpha)[None])
                run = spread(cur[regs - 1, SUBLANES - 1:SUBLANES, :])
                cur = cur.reshape(size, LANES)
                voc = lax.broadcasted_iota(jnp.int32, (size, LANES), 0) + v0
                hit = jnp.where(voc == tgt, cur, 0.0).reshape(regs, SUBLANES, LANES)
                tacc = tacc * alpha + jnp.sum(hit, axis=0)
                c_ref[v0:v0 + size, lanes] = cur
                mh_v[v0 // SEG:v0 // SEG + 1, lanes] = m[0:1, :]
            st_v[0, :, lanes] = m
            st_v[1, :, lanes] = run
            st_v[2, :, lanes] = tacc

    def before(k):
        return lax.rem(me + n - k, n)

    def combine(tgt, m_own, s_own, t_own, m_of, s_of, t_of):
        gm = m_own
        for k in range(1, n):
            gm = jnp.maximum(gm, m_of(k))
        f = exp_of(m_own - gm)
        sc = s_own * f
        total, prev = sc, jnp.zeros_like(sc)
        hit = jnp.where((me + 1) * width <= tgt, sc, 0.0)
        scales = [f]
        for k in range(1, n):
            f = exp_of(m_of(k) - gm)
            sc = s_of(k) * f
            src = before(k)
            total = total + sc
            prev = prev + jnp.where(src < me, sc, 0.0)
            hit = hit + jnp.where((src + 1) * width <= tgt, sc, 0.0)
            scales.append(f)
        return gm, total, prev, hit, scales

    def put_ab(rg, part, gm, total, prev):
        lanes = slice(rg * LANES, (rg + 1) * LANES)
        ab_ref[n_seg:n_seg + 1, lanes] = prev / total
        for r0, seg in part:
            ab_ref[r0:r0 + seg.shape[0], lanes] = exp_of(seg - gm) / total

    each(lambda k: greet(k, 0))
    start_all()
    st_v[...] = st_ref[...]
    wait_h()
    wait_w(0)
    pl.semaphore_wait(barrier, n - 1)
    each(lambda k: early_copy(k).start())
    dot_tile(0)
    for s in range(1, n_tail):
        wait_w(s)
    for s in range(1, n_tail):
        epilogue(s - 1)
        dot_tile(s)
    epilogue(n_tail - 1)
    late_v[0:n_mixed, :] = stat_ref[n_early:n_early + n_mixed, :]
    for g in range(groups):
        lanes = slice(g * LANES, (g + 1) * LANES)
        late_v[n_mixed + g:n_mixed + g + 1, :] = st_v[0, 0:1, lanes]
        late_v[n_mixed + groups + g:n_mixed + groups + g + 1, :] = st_v[1, 0:1, lanes]
        late_v[n_mixed + 2 * groups + g:n_mixed + 2 * groups + g + 1, :] = (
            all_sublanes(jnp.add, st_v[2, :, lanes])[0:1, :])
    each(lambda k: late_copy(k).start())

    each(lambda k: early_copy(k).wait_recv())
    tgt_a = tgt_ref[0:done, :]
    gm, total, prev, hit, scales = combine(
        tgt_a, stat_ref[0:done, :], stat_ref[done:2 * done, :], None,
        lambda k: recv_a[k - 1, 0:done, :], lambda k: recv_a[k - 1, done:2 * done, :], None)
    n_t = done - n_mixed
    hit_a = hit[0:n_t] + stat_ref[2 * done:2 * done + n_t, :] * scales[0][0:n_t]
    for k in range(1, n):
        hit_a = hit_a + recv_a[k - 1, 2 * done:2 * done + n_t, :] * scales[k][0:n_t]
    ct_ref[0:n_t, :] = hit_a / total[0:n_t]
    for rg in range(done):
        put_ab(rg, [(0, mh_ref[:, rg * LANES:(rg + 1) * LANES])],
               gm[rg:rg + 1], total[rg:rg + 1], prev[rg:rg + 1])

    each(lambda k: late_copy(k).wait_recv())
    hit_b = hit[n_t:] + late_v[0:n_mixed, :] * scales[0][n_t:]
    for k in range(1, n):
        hit_b = hit_b + recv_b[k - 1, 0:n_mixed, :] * scales[k][n_t:]
    ct_ref[n_t:done, :] = hit_b / total[n_t:]

    q = [n_mixed + i * groups for i in range(4)]
    gm, total, prev, hit, scales = combine(
        tgt_ref[done:, :], late_v[q[0]:q[1], :], late_v[q[1]:q[2], :], None,
        lambda k: recv_b[k - 1, q[0]:q[1], :], lambda k: recv_b[k - 1, q[1]:q[2], :], None)
    hit = hit + late_v[q[2]:q[3], :] * scales[0]
    for k in range(1, n):
        hit = hit + recv_b[k - 1, q[2]:q[3], :] * scales[k]
    ct_ref[done:, :] = hit / total
    for g in range(groups):
        rg = done + g
        put_ab(rg, [(0, mh_ref[0:head_seg, rg * LANES:(rg + 1) * LANES]),
                    (head_seg, mh_v[:, g * LANES:(g + 1) * LANES])],
               gm[g:g + 1], total[g:g + 1], prev[g:g + 1])
    each(lambda k: early_copy(k).wait_send())
    each(lambda k: late_copy(k).wait_send())


def table_kernel(c_ref, c2_ref, ab_ref, ct_ref, out_hbm, ct_out, stage, sem):
    width, rows = out_hbm.shape
    ct_out[...] = ct_ref[...]
    n_seg = pl.cdiv(width, SEG)
    head = HEAD_CHUNKS * CHUNK

    def copy(t):
        v = pl.ds(t * SEG, min(SEG, width - t * SEG))
        return pltpu.make_async_copy(stage.at[v, :], out_hbm.at[v, :], sem.at[t])

    for t in range(n_seg):
        v0 = t * SEG
        size = min(SEG, width - v0)
        split = rows if v0 < head else rows - UNIT
        lo, hi = slice(0, split), slice(split, rows)
        stage[v0:v0 + size, lo] = c_ref[v0:v0 + size, lo] * ab_ref[t:t + 1, lo] + ab_ref[n_seg:n_seg + 1, lo]
        if split < rows:
            stage[v0:v0 + size, hi] = (c2_ref[v0 - head:v0 - head + size, :] * ab_ref[t:t + 1, hi]
                                       + ab_ref[n_seg:n_seg + 1, hi])
        copy(t).start()
    for t in range(n_seg):
        copy(t).wait()


def solution(mesh):
    n = mesh.shape["vp"]

    def local_fn(h_rows, w_cols, tau_rows, tgt_rows):
        rows, depth = h_rows.shape
        width = w_cols.shape[1]
        n_rg = rows // LANES
        n_seg = pl.cdiv(width, SEG)
        ab_rows = pl.cdiv(n_seg + 1, SUBLANES) * SUBLANES
        vmem = pl.BlockSpec(memory_space=pltpu.VMEM)
        hbm = pl.BlockSpec(memory_space=pl.ANY)
        tau2, tgt2 = tau_rows.reshape(n_rg, LANES), tgt_rows.reshape(n_rg, LANES)
        half = rows // 2
        head = HEAD_CHUNKS * CHUNK
        tail = width - head
        done = n_rg - UNIT // LANES
        n_early = 3 * done // SUBLANES * SUBLANES
        n_late = 3 * n_rg - n_early
        f32 = jnp.float32
        wt = w_cols.T
        c, stat, st, mh = pl.pallas_call(
            main_kernel,
            name="main_kernel",
            out_shape=(pltpu.VMEM((width, rows), f32),
                       pltpu.VMEM((3 * n_rg, LANES), f32),
                       pltpu.VMEM((3, SUBLANES, UNIT), f32),
                       pltpu.VMEM((n_seg, rows), f32)),
            in_specs=[hbm, hbm, vmem, vmem],
            out_specs=(vmem,) * 4,
            scratch_shapes=[
                pltpu.VMEM((head, depth), jnp.bfloat16),
                pltpu.VMEM((tail, depth), jnp.bfloat16),
                pltpu.VMEM((half, depth), jnp.bfloat16),
                pltpu.VMEM((half, depth), jnp.bfloat16),
                pltpu.VMEM((2, CHUNK, half), f32),
                pltpu.VMEM((SUBLANES, rows), f32),
                pltpu.VMEM((SUBLANES, rows), f32),
                pltpu.VMEM((SUBLANES, rows), f32),
                pltpu.SemaphoreType.DMA((pl.cdiv(width, CHUNK),)),
                pltpu.SemaphoreType.DMA((2,)),
            ],
            compiler_params=pltpu.CompilerParams(vmem_limit_bytes=45 * 1024 * 1024),
        )(wt, h_rows, tau2, tgt2)
        in_vmem = lambda *xs: [pltpu.with_memory_space_constraint(x, pltpu.VMEM) for x in xs]
        c, stat, st, mh = in_vmem(c, stat, st, mh)
        c2, ab, ct = pl.pallas_call(
            functools.partial(tail_kernel, n, width),
            name="tail_kernel",
            out_shape=(pltpu.VMEM((tail, UNIT), f32),
                       pltpu.VMEM((ab_rows, rows), f32),
                       pltpu.VMEM((n_rg, LANES), f32)),
            in_specs=[hbm, hbm] + [vmem] * 5,
            out_specs=(vmem,) * 3,
            scratch_shapes=[
                pltpu.VMEM((tail, depth), jnp.bfloat16),
                pltpu.VMEM((UNIT, depth), jnp.bfloat16),
                pltpu.SemaphoreType.DMA((pl.cdiv(tail, CHUNK),)),
                pltpu.SemaphoreType.DMA,
                pltpu.VMEM((2, CHUNK, UNIT), f32),
                pltpu.VMEM((3, SUBLANES, UNIT), f32),
                pltpu.VMEM((pl.cdiv(tail, SEG), UNIT), f32),
                pltpu.VMEM((n_late, LANES), f32),
                pltpu.VMEM((n - 1, n_early, LANES), f32),
                pltpu.VMEM((n - 1, n_late, LANES), f32),
            ] + [pltpu.SemaphoreType.DMA((n - 1,))] * 4,
            compiler_params=pltpu.CompilerParams(
                collective_id=0, has_side_effects=True, vmem_limit_bytes=20 * 1024 * 1024),
        )(*(pltpu.with_memory_space_constraint(x, pltpu.HBM) for x in (wt, h_rows)), tau2, tgt2, stat, st, mh)
        table, ct2 = pl.pallas_call(
            table_kernel,
            name="table_kernel",
            out_shape=(jax.ShapeDtypeStruct((width, rows), jnp.float32),
                       jax.ShapeDtypeStruct((n_rg, LANES), jnp.float32)),
            in_specs=[vmem] * 4,
            out_specs=(hbm, vmem),
            scratch_shapes=[pltpu.VMEM((width, rows), jnp.float32),
                            pltpu.SemaphoreType.DMA((n_seg,))],
            compiler_params=pltpu.CompilerParams(vmem_limit_bytes=20 * 1024 * 1024),
        )(c, *in_vmem(c2, ab, ct))
        return table.T, ct2.reshape(rows)

    return jax.shard_map(
        local_fn,
        mesh=mesh,
        in_specs=(P("dp", None), P(None, "vp"), P("dp"), P("dp")),
        out_specs=(P("dp", "vp"), P("dp")),
        check_vma=False,
    )
```
